32 devices in a mesh: section: 2 (over y), rep: 4 (over z), sub: 4 (over x, core).
Axes of the slice: x: 2, y: 2, z: 4, core: 2. Of those that a mesh axis runs over, the one named last changes fastest.
Arguments:
- token_ids: int32 [8, 512], P(None, ('rep', 'sub')), may hold values from 0 to 255
- target_ids: int32 [8, 512], P(None, ('rep', 'sub')), may hold values from 0 to 255
- embedding: bfloat16 [256, 2048], P(('rep', 'sub')), may hold values from -3 to 3
- section_weight: bfloat16 [2, 2048, 2048], P('section', ('rep', 'sub')), may hold values from -0.125 to 0.125
- section_gain: float32 [2, 2048], P('section'), may hold values from 0.1 to 1.9
- final_gain: float32 [2048], replicated, may hold values from 0.5 to 1.5
Outputs:
- weight_grad: float32 [2, 2048, 2048], P('section', ('rep', 'sub'))
- gain_grad: float32 [2, 2048], P('section')
- embed_grad: float32 [256, 2048], P(('section', 'rep', 'sub'))
- final_grad: float32 [2048], replicated
The draws below stay inside these ranges and needn't reach their ends.
All inputs are finite; a program needn't handle non-finite values.
Results may differ from the reference program's by a relative error of at most 0.024.
Values may be sent and summed in bfloat16 or wider, within the bound.
A program may use at most 64 MiB of HBM per device.

```python
import math
import jax
import jax.numpy as jnp
import numpy as np
from jax import lax

D = 2048
VOCAB = 256
MICRO = 8
SECTIONS = 2
TOKENS = 512
N_SECTION = 2


def set_ends(entries, key, low, largest):
    index_at = [jax.random.randint(jax.random.fold_in(key, axis), (), 0, length) for axis, length in enumerate(entries.shape)]
    main_axis = entries.shape.index(max(entries.shape))
    neighbour = index_at[:main_axis] + [(index_at[main_axis] + 1) % entries.shape[main_axis]] + index_at[main_axis + 1:]
    return entries.at[tuple(index_at)].set(low).at[tuple(neighbour)].set(largest)


def block_levels(key, extent, pieces, low, top_value):
    level = 1.0
    for axis_at, shards_of in pieces:
        draws = jax.random.uniform(jax.random.fold_in(jax.random.fold_in(key, 6), axis_at), (shards_of,), jnp.float32, low / len(pieces), top_value / len(pieces))
        level = level * jnp.repeat(jnp.exp(draws), extent[axis_at] // shards_of).reshape((-1,) + (1,) * (len(extent) - 1 - axis_at))
    return level


def cumulative_ranks(amount, slope):
    portions = [(1 << 20) // math.isqrt(grade ** slope) + 1 for grade in range(1, amount + 1)]
    width = 1 + sum(portions) // (1 << 30)
    return np.cumsum(np.array([max(1, weight // width) for weight in portions]))


def ranked(own_key, extent, count, lean):
    grid = cumulative_ranks(count, lean)
    pick = jax.random.randint(jax.random.fold_in(own_key, 1), extent, 0, int(grid[count - 1]))
    rank = jnp.searchsorted(jnp.asarray(grid, jnp.int32), pick, side="right")
    return jax.random.permutation(jax.random.fold_in(own_key, 2), count)[rank].astype(jnp.int32)


def centred(rng, shape, spread, most, split=(), kind=jnp.bfloat16):
    drawn = spread * jax.random.normal(rng, shape, jnp.float32)
    if split:
        drawn = drawn * block_levels(rng, shape, split, -0.22, 0.18)
    return jnp.clip(drawn, -most, most).astype(kind)


def setup_inputs(seed: int = 0) -> dict:
    key_list = jax.random.split(jax.random.key(seed), 7)
    return {
        "token_ids": set_ends(ranked(key_list[0], (MICRO, TOKENS), VOCAB, 2), jax.random.fold_in(key_list[0], 3), 0, VOCAB - 1).astype(jnp.int32),
        "target_ids": set_ends(ranked(key_list[1], (MICRO, TOKENS), VOCAB, 1), jax.random.fold_in(key_list[1], 3), 0, VOCAB - 1).astype(jnp.int32),
        "embedding": centred(key_list[2], (VOCAB, D), 0.25, 3.0, ((0, 16),)),
        "section_weight": centred(key_list[3], (SECTIONS, D, D), D ** -0.5, 0.125, ((0, 2), (1, 16))),
        "section_gain": jnp.clip(1.0 + 0.18 * jax.random.normal(key_list[4], (SECTIONS, D), jnp.float32), 0.1, 1.9),
        "final_gain": jnp.clip(1.0 + 0.1 * jax.random.normal(key_list[5], (D,), jnp.float32), 0.5, 1.5),
    }


epsilon = 1e-06
gelu_coef = 0.7978845608028654
cube_coef = 0.044715

def gelu(pre_act):
    return 0.5 * pre_act * (1.0 + jnp.tanh(gelu_coef * (pre_act + cube_coef * pre_act * pre_act * pre_act)))

def gelu_slope(pre_act):
    inside = gelu_coef * (pre_act + cube_coef * pre_act * pre_act * pre_act)
    tangent = jnp.tanh(inside)
    return 0.5 * (1.0 + tangent) + 0.5 * pre_act * (1.0 - tangent * tangent) * gelu_coef * (1.0 + 3.0 * cube_coef * pre_act * pre_act)

def normalize(residual, gain_row):
    values = residual.astype(jnp.float32)
    scale_inv = lax.rsqrt(lax.optimization_barrier(jnp.mean(values * values, axis=-1, keepdims=True)) + epsilon)
    normed = values * scale_inv
    return (normed, scale_inv, (normed * gain_row).astype(jnp.bfloat16))

def norm_back(grad_norm, normed, scale_inv, gain_row):
    grad_unit = grad_norm * gain_row
    grad_in = scale_inv * (grad_unit - normed * lax.optimization_barrier(jnp.mean(grad_unit * normed, axis=-1, keepdims=True)))
    return (grad_in, lax.optimization_barrier(jnp.sum(grad_norm * normed, axis=0)))

def reference(token_ids, target_ids, embedding, section_weight, section_gain, final_gain):
    vocab_iota = jnp.arange(VOCAB, dtype=jnp.int32)
    onehot_in = (token_ids.reshape(-1)[:, None] == vocab_iota[None, :]).astype(jnp.bfloat16)
    residual = jnp.dot(onehot_in, embedding, preferred_element_type=jnp.float32).astype(jnp.bfloat16)
    saved = []
    for layer_index in range(N_SECTION):
        normed, scale_inv, rounded = normalize(residual, section_gain[layer_index])
        pre_act = jnp.dot(rounded, section_weight[layer_index], preferred_element_type=jnp.float32)
        saved.append((residual, rounded, pre_act))
        residual = (residual.astype(jnp.float32) + gelu(pre_act)).astype(jnp.bfloat16)
    normed, scale_inv, final_rows = normalize(residual, final_gain)
    logit_scale = float(D) ** (-0.5)
    contract_last = (((1,), (1,)), ((), ()))
    contract_first = (((0,), (0,)), ((), ()))
    logits = lax.dot_general(final_rows, embedding, contract_last, preferred_element_type=jnp.float32) * logit_scale
    exp_logit = jnp.exp(logits)
    probability = exp_logit / lax.optimization_barrier(jnp.sum(exp_logit, axis=-1, keepdims=True))
    onehot_out = (target_ids.reshape(-1)[:, None] == vocab_iota[None, :]).astype(jnp.float32)
    grad_logit = ((probability - onehot_out) * logit_scale).astype(jnp.bfloat16)
    embed_head = lax.dot_general(grad_logit, final_rows, contract_first, preferred_element_type=jnp.float32)
    grad_final = jnp.dot(grad_logit, embedding, preferred_element_type=jnp.float32)
    grad_in, final_grad = norm_back(grad_final, normed, scale_inv, final_gain)
    grad_residual = grad_in.astype(jnp.bfloat16)
    weight_list = []
    gain_list = []
    for layer_index in reversed(range(N_SECTION)):
        residual_in, rounded, pre_act = saved[layer_index]
        grad_float = grad_residual.astype(jnp.float32)
        grad_pre = (grad_float * gelu_slope(pre_act)).astype(jnp.bfloat16)
        weight_list.append(lax.dot_general(rounded, grad_pre, contract_first, preferred_element_type=jnp.float32))
        grad_norm = lax.dot_general(grad_pre, section_weight[layer_index], contract_last, preferred_element_type=jnp.float32)
        normed, scale_inv, rounded_again = normalize(residual_in, section_gain[layer_index])
        grad_in, gain_part = norm_back(grad_norm, normed, scale_inv, section_gain[layer_index])
        gain_list.append(gain_part)
        grad_residual = (grad_float + grad_in).astype(jnp.bfloat16)
    embed_in = lax.dot_general(onehot_in, grad_residual, contract_first, preferred_element_type=jnp.float32)
    weight_grad = jnp.stack(weight_list[::-1])
    gain_grad = jnp.stack(gain_list[::-1])
    return (weight_grad, gain_grad, embed_in + embed_head, final_grad)
```

```python
import functools
import jax
import jax.numpy as jnp
from jax import lax
from jax.experimental import pallas as pl
from jax.experimental.pallas import tpu as pltpu
from jax.sharding import PartitionSpec as P

epsilon = 1e-06
gelu_coef = 0.7978845608028654
cube_coef = 0.044715


def passed_along(value, axis, steps):
    count = lax.axis_size(axis)
    initial, last = (max(0, -steps), min(count, count - steps))
    return lax.ppermute(value, axis, [(source, source + steps) for source in range(initial, last)])


def gelu(pre_act):
    return (
        0.5
        * pre_act
        * (1.0 + jnp.tanh(gelu_coef * (pre_act + cube_coef * pre_act * pre_act * pre_act)))
    )


def gelu_slope(pre_act):
    inside = gelu_coef * (pre_act + cube_coef * pre_act * pre_act * pre_act)
    tangent = jnp.tanh(inside)
    return 0.5 * (1.0 + tangent) + 0.5 * pre_act * (1.0 - tangent * tangent) * gelu_coef * (
        1.0 + 3.0 * cube_coef * pre_act * pre_act
    )


def normalize(residual, gain_row):
    values = residual.astype(jnp.float32)
    scale_inv = lax.rsqrt(jnp.mean(values * values, axis=-1, keepdims=True) + epsilon)
    normed = values * scale_inv
    return (normed, scale_inv, (normed * gain_row).astype(jnp.bfloat16))


def norm_back(grad_norm, normed, scale_inv, gain_row):
    grad_unit = grad_norm * gain_row
    grad_in = scale_inv * (
        grad_unit - normed * jnp.mean(grad_unit * normed, axis=-1, keepdims=True)
    )
    return (grad_in, jnp.sum(grad_norm * normed, axis=0))


def pick_slot(buffer, slot_index):
    return lax.dynamic_index_in_dim(buffer, slot_index, 0, keepdims=False)


def place_slot(buffer, update, slot_index):
    return lax.dynamic_update_index_in_dim(buffer, update, slot_index, 0)


def pipeline_body(token_ids, target_ids, embedding, section_weight, section_gain, final_gain):
    sections = lax.axis_size("section")
    position = lax.axis_index("section")
    micro_count = token_ids.shape[0]
    row_count = token_ids.shape[1]
    features = embedding.shape[1]
    group_size = lax.axis_size(("rep", "sub"))
    vocab_rows = embedding.shape[0] * group_size
    tick_count = micro_count + sections - 1
    contract_last = (((1,), (1,)), ((), ()))
    contract_first = (((0,), (0,)), ((), ()))
    vocab_table = lax.all_gather(embedding, ("rep", "sub"), axis=0, tiled=True)
    weight = lax.all_gather(section_weight, ("rep", "sub"), axis=1, tiled=True)[0]
    gain_row = section_gain[0]
    is_first = position == 0
    is_last = position == sections - 1
    vocab_iota = jnp.arange(vocab_rows, dtype=jnp.int32)
    onehot_in = (token_ids.reshape(-1)[:, None] == vocab_iota[None, :]).astype(jnp.bfloat16)
    embedded = jnp.dot(onehot_in, vocab_table, preferred_element_type=jnp.float32).astype(
        jnp.bfloat16
    )
    embedded = embedded.reshape(micro_count, row_count, features)
    empty_rows = jnp.zeros((row_count, features), jnp.bfloat16)
    zeros_stash = jnp.zeros((micro_count, row_count, features), jnp.bfloat16)
    zeros_pre = jnp.zeros((micro_count, row_count, features), jnp.float32)

    def forward_tick(carried, tick_index):
        arrived = carried[0]
        buffers = carried[1:]
        offset = tick_index - position
        active = (offset >= 0) & (offset < micro_count)
        slot_index = jnp.clip(offset, 0, micro_count - 1)
        residual = jnp.where(is_first, pick_slot(embedded, slot_index), arrived)

        def forward_compute(kept_activations):
            input_list, rounded_list, preactivation_list, output_list = kept_activations
            normed, scale_inv, rounded = normalize(residual, gain_row)
            pre_act = jnp.dot(rounded, weight, preferred_element_type=jnp.float32)
            returned_value = (residual.astype(jnp.float32) + gelu(pre_act)).astype(jnp.bfloat16)
            kept_activations = (
                place_slot(input_list, residual, slot_index),
                place_slot(rounded_list, rounded, slot_index),
                place_slot(preactivation_list, pre_act, slot_index),
                place_slot(output_list, returned_value, slot_index),
            )
            return (kept_activations, returned_value)

        def forward_bypass(kept_activations):
            return (kept_activations, empty_rows)

        buffers, returned_value = lax.cond(active, forward_compute, forward_bypass, buffers)
        arrived = passed_along(returned_value, "section", 1)
        return ((arrived,) + buffers, None)

    start_state = (empty_rows, zeros_stash, zeros_stash, zeros_pre, zeros_stash)
    final_state, unused_out = lax.scan(
        forward_tick, start_state, jnp.arange(tick_count, dtype=jnp.int32)
    )
    input_list, rounded_list, preactivation_list, output_list = final_state[1:]
    logit_scale = float(features) ** (-0.5)

    def head(finals):
        normed, scale_inv, final_rows = normalize(finals, final_gain)
        logits = (
            lax.dot_general(
                final_rows, vocab_table, contract_last, preferred_element_type=jnp.float32
            )
            * logit_scale
        )
        exp_logit = jnp.exp(logits)
        probability = exp_logit / jnp.sum(exp_logit, axis=-1, keepdims=True)
        onehot_out = (target_ids.reshape(-1)[:, None] == vocab_iota[None, :]).astype(jnp.float32)
        grad_logit = ((probability - onehot_out) * logit_scale).astype(jnp.bfloat16)
        embed_head = lax.dot_general(
            grad_logit, final_rows, contract_first, preferred_element_type=jnp.float32
        )
        grad_final = jnp.dot(grad_logit, vocab_table, preferred_element_type=jnp.float32)
        grad_in, final_part = norm_back(grad_final, normed, scale_inv, final_gain)
        grad_top = grad_in.astype(jnp.bfloat16).reshape(micro_count, row_count, features)
        return (embed_head, grad_top, final_part)

    def no_head(finals):
        return (
            jnp.zeros((vocab_rows, features), jnp.float32),
            zeros_stash,
            jnp.zeros((features,), jnp.float32),
        )

    embed_head, grad_top, final_part = lax.cond(
        is_last, head, no_head, output_list.reshape(-1, features)
    )

    def backward_tick(carried, tick_index):
        arrived = carried[0]
        buffers = carried[1:]
        offset = tick_index - (sections - 1 - position)
        active = (offset >= 0) & (offset < micro_count)
        slot_index = jnp.clip(offset, 0, micro_count - 1)
        grad_out = jnp.where(is_last, pick_slot(grad_top, slot_index), arrived)

        def backward_compute(kept_activations):
            preactivation_gradients, first_row_gradients, gain_accumulated = kept_activations
            grad_float = grad_out.astype(jnp.float32)
            grad_pre = (grad_float * gelu_slope(pick_slot(preactivation_list, slot_index))).astype(
                jnp.bfloat16
            )
            grad_norm = lax.dot_general(
                grad_pre, weight, contract_last, preferred_element_type=jnp.float32
            )
            normed, scale_inv, rounded = normalize(pick_slot(input_list, slot_index), gain_row)
            grad_in, gain_part = norm_back(grad_norm, normed, scale_inv, gain_row)
            sent_output = (grad_float + grad_in).astype(jnp.bfloat16)
            kept_activations = (
                place_slot(preactivation_gradients, grad_pre, slot_index),
                place_slot(first_row_gradients, sent_output, slot_index),
                gain_accumulated + gain_part,
            )
            return (kept_activations, sent_output)

        def backward_bypass(kept_activations):
            return (kept_activations, empty_rows)

        buffers, sent_output = lax.cond(active, backward_compute, backward_bypass, buffers)
        arrived = passed_along(sent_output, "section", -1)
        return ((arrived,) + buffers, None)

    back_state = (empty_rows, zeros_stash, zeros_stash, jnp.zeros((features,), jnp.float32))
    back_final, unused_back = lax.scan(
        backward_tick, back_state, jnp.arange(tick_count, dtype=jnp.int32)
    )
    preactivation_gradients, first_row_gradients, gain_accumulated = back_final[1:]
    pres_flat = preactivation_gradients.reshape(-1, features)
    rounded_flat = rounded_list.reshape(-1, features)
    weight_part = lax.psum_scatter(
        lax.dot_general(
            rounded_flat, pres_flat, contract_first, preferred_element_type=jnp.float32
        ).astype(jnp.bfloat16),
        ("rep", "sub"),
        scatter_dimension=0,
        tiled=True,
    ).astype(jnp.float32)
    gain_total = lax.psum(gain_accumulated, ("rep", "sub"))
    final_total = lax.psum(final_part, ("section", "rep", "sub"))
    embed_in = lax.dot_general(
        onehot_in,
        first_row_gradients.reshape(-1, features),
        contract_first,
        preferred_element_type=jnp.float32,
    )
    contribution = jnp.where(is_first, embed_in, 0.0) + embed_head
    embed_total = lax.psum_scatter(
        contribution, ("section", "rep", "sub"), scatter_dimension=0, tiled=True
    )
    return (weight_part[None], gain_total[None], embed_total, final_total)


LANES = 128
SUBLANES = 8
MESH = pl.DeviceIdType.MESH
over_last = (((1,), (1,)), ((), ()))
over_first = (((0,), (0,)), ((), ()))


def matmul(left, right, dims=(((1,), (0,)), ((), ()))):
    return lax.dot_general(left, right, dims, preferred_element_type=jnp.float32)


def row_kernel(
    reps,
    ids_ref,
    emb_ref,
    w_ref,
    gain_ref,
    final_ref,
    weight_out,
    gain_out,
    embed_out,
    final_out,
    emb,
    ids,
    wc,
    wr,
    gains,
    counts,
    x0,
    x1,
    x2,
    normed,
    top,
    act,
    dx2,
    dx1,
    da,
    near,
    qt,
    hg,
    hg_in,
    dn0,
    dn0_in,
    g0,
    g0_in,
    part,
    part_in,
    scale,
    send_sem,
    w_recv,
    emb_recv,
    ids_recv,
    act_recv,
    wr_recv,
    misc_recv,
    dn0_recv,
    g0_recv,
):
    y, z, sub = (lax.axis_index(name) for name in ("section", "rep", "sub"))
    x, core = sub // 2, sub % 2
    chips = 4 * reps
    members = 4 * reps
    own_k = z * 4 + sub
    features = emb.shape[1]
    vocab = emb.shape[0]
    half = vocab // 2
    width = features // chips
    depth = features // members
    group = vocab // (2 * members)
    held = vocab // members
    blocks = features // LANES
    logit_scale = float(features) ** (-0.5)

    def device(dy, dz, dx, other_core=False):
        place = {"section": 1 - y if dy else y, "rep": lax.rem(z + dz, reps)}
        across = 1 - x if dx else x
        place["sub"] = across * 2 + (1 - core if other_core else core)
        return place

    partner = device(0, 0, 0, True)

    def chip_of(ya, za, xa):
        return za * 4 + xa * 2 + ya

    own_f = chip_of(y, z, x)

    def cols(index, size=width):
        return pl.ds(pl.multiple_of(index * size, size), size)

    barrier = pltpu.get_barrier_semaphore()
    count = 0
    for dy in range(2):
        for dz in range(reps):
            for dx in range(2):
                for dc in range(2):
                    if dy or dz or dx or dc:
                        pl.semaphore_signal(
                            barrier, inc=1, device_id=device(dy, dz, dx, bool(dc)), device_id_type=MESH
                        )
                        count += 1
    pl.semaphore_wait(barrier, count)

    numbers = [0]
    sent = []

    def message(source, target, recv, place):
        number = numbers[0]
        numbers[0] += 1
        return pltpu.make_async_remote_copy(
            src_ref=source,
            dst_ref=target,
            send_sem=send_sem.at[number],
            recv_sem=recv,
            device_id=place,
            device_id_type=MESH,
        )

    def send(source, target, recv, place, when=None):
        copy = message(source, target, recv, place)
        sent.append((when, copy))
        if when is None:
            copy.start()
        else:
            pl.when(when)(copy.start)

    def arrived(target, recv):
        pltpu.make_async_copy(target, target, recv).wait()

    below, above = z, reps - 1 - z
    both = jnp.minimum(below, above)
    z_near = []
    for step in range(1, reps):
        paired = step <= 2 * both
        hop = jnp.where(paired, (step + 1) // 2, step - both)
        up = jnp.where(paired, step % 2 == 1, above > below)
        z_near.append(jnp.where(up, z + hop, z - hop))

    def at(dy, za, dx, other_core=False):
        place = device(dy, 0, dx, other_core)
        place["rep"] = za
        return place

    gains[y] = gain_ref[...]
    send(gain_ref, gains.at[y], misc_recv.at[0], device(1, 0, 0))

    def weight_columns(layer):
        rows = cols(own_k, depth)
        for za in reversed(z_near + [z]):
            for dy, dx in ((1, 1), (1, 0), (0, 1), (0, 0)):
                if za is z and not dy and not dx:
                    continue
                there = chip_of(1 - y if dy else y, za, 1 - x if dx else x)
                send(
                    w_ref.at[:, cols(there)],
                    wc.at[layer, rows],
                    w_recv.at[layer * members + own_k],
                    at(dy, za, dx),
                    y == layer,
                )
        own = w_ref.at[:, cols(own_f)]
        send(own, wc.at[layer, rows], w_recv.at[layer * members + own_k], partner, y == layer)

    weight_columns(0)
    wc[y, cols(own_k, depth)] = w_ref[:, cols(own_f)]

    own_rows = cols(own_k, held)
    emb[own_rows] = emb_ref[...]
    for za in reversed(z_near):
        send(emb_ref, emb.at[own_rows], emb_recv.at[own_k], at(0, za, 0))
    send(emb_ref, emb.at[own_rows], emb_recv.at[own_k], device(0, 0, 1))
    send(emb_ref, emb.at[own_rows], emb_recv.at[own_k], partner)
    for za in z_near:
        k = za * 4 + sub
        block = emb.at[cols(k, held)]
        arrived(block, emb_recv.at[k])
        send(block, block, emb_recv.at[k], device(0, 0, 1))
        send(block, block, emb_recv.at[k], partner)
    weight_columns(1)

    keeper = core == y
    send(w_ref, wr.at[y], wr_recv.at[y], partner, keeper)
    send(w_ref, wr.at[y], wr_recv.at[y], device(1, 0, 0), jnp.logical_not(keeper))

    @pl.when(keeper)
    def _():
        wr[y] = w_ref[...]

    ids[own_k] = ids_ref[...]
    for dz in reversed(range(reps)):
        for dx in (1, 0):
            for dc in (1, 0):
                if dz or dx or dc:
                    send(ids_ref, ids.at[own_k], ids_recv.at[own_k], device(0, dz, dx, bool(dc)))

    for za in [z] + z_near:
        k = za * 4 + (1 - x) * 2 + core
        block = emb.at[cols(k, held)]
        arrived(block, emb_recv.at[k])
        send(block, block, emb_recv.at[k], partner)
    for za in [z] + z_near:
        for xa in (x, 1 - x):
            k = za * 4 + xa * 2 + 1 - core
            arrived(emb.at[cols(k, held)], emb_recv.at[k])

    def own_vocab(shape):
        index = lax.broadcasted_iota(jnp.int32, shape, 0)
        return 2 * index - (index & (group - 1)) + core * group

    pick = (
        lax.broadcasted_iota(jnp.int32, (half, vocab), 1) == own_vocab((half, vocab))
    ).astype(jnp.float32).astype(jnp.bfloat16)

    def sweep(body, start):
        return lax.fori_loop(0, blocks, lambda j, carry: body(cols(j, LANES), carry), start)

    flat = jnp.zeros((half, LANES), jnp.float32)

    def scale_inv(squares):
        mean = jnp.sum(squares, axis=-1, keepdims=True) * (1.0 / features)
        return jnp.broadcast_to(lax.rsqrt(mean + epsilon), (half, LANES))

    def mean_of(total):
        mean = jnp.sum(total, axis=-1, keepdims=True) * (1.0 / features)
        return jnp.broadcast_to(mean, (half, LANES))

    def look_up(block, squares):
        values = matmul(pick, emb[:, block])
        x0[:, block] = values.astype(jnp.bfloat16)
        return squares + values * values

    scale[0] = scale_inv(sweep(look_up, flat))
    arrived(gains.at[1 - y], misc_recv.at[0])

    def norm_into(target, source, slot, gain):
        def body(block, carry):
            unit = source[:, block].astype(jnp.float32) * scale[slot]
            target[:, block] = (unit * gain[:, block]).astype(jnp.bfloat16)
            return carry

        sweep(body, 0)

    norm_into(normed.at[0], x0, 0, gains.at[0])

    def near_rows(layer):
        rows = cols(core, half)

        @pl.when(y == layer)
        def _():
            near[rows] = normed[layer, :, cols(own_k, depth)]

        send(
            normed.at[layer, :, cols(z * 4 + x * 2 + 1 - core, depth)],
            near.at[rows],
            misc_recv.at[1],
            partner,
            y == layer,
        )

    def gather_columns(layer):
        for za in [z] + z_near:
            for dx in (0, 1):
                k = za * 4 + (1 - x if dx else x) * 2 + core
                block = wc.at[layer, cols(k, depth)]
                recv = w_recv.at[layer * members + k]
                if za is z and not dx:

                    @pl.when(y != layer)
                    def _():
                        arrived(block, recv)

                    send(block, block, recv, partner, y != layer)
                else:
                    arrived(block, recv)
                    send(block, block, recv, partner)

    def columns_ready(layer):
        for za in range(reps):
            for xa in range(2):
                k = za * 4 + xa * 2 + 1 - core
                arrived(wc.at[layer, cols(k, depth)], w_recv.at[layer * members + k])

    def spread(slot, block, f):
        recv = act_recv.at[slot * chips + f]
        for dy, dx in ((1, 1), (1, 0), (0, 1)):
            send(block, block, recv, device(dy, 0, dx))

    def gather_start(slot):
        block = act.at[slot, :, cols(own_f)]
        for za in reversed(z_near):
            send(block, block, act_recv.at[slot * chips + own_f], at(0, za, 0))
        spread(slot, block, own_f)

    def gather_forward(slot):
        for za in z_near:
            f = chip_of(y, za, x)
            block = act.at[slot, :, cols(f)]
            arrived(block, act_recv.at[slot * chips + f])
            spread(slot, block, f)

    def gather_finish(slot):
        for za in [z] + z_near:
            for dy, dx in ((1, 0), (0, 1), (1, 1)):
                f = chip_of(1 - y if dy else y, za, 1 - x if dx else x)
                arrived(act.at[slot, :, cols(f)], act_recv.at[slot * chips + f])

    def inner(pre_act):
        return jnp.tanh(gelu_coef * (pre_act + cube_coef * pre_act * pre_act * pre_act))

    def slope(pre_act):
        tangent = inner(pre_act)
        return 0.5 * (1.0 + tangent) + 0.5 * pre_act * (1.0 - tangent * tangent) * gelu_coef * (
            1.0 + 3.0 * cube_coef * pre_act * pre_act
        )

    def layer_out(target, source, pre):
        def body(block, squares):
            pre_act = pre[:, block].astype(jnp.float32)
            values = source[:, block].astype(jnp.float32) + 0.5 * pre_act * (1.0 + inner(pre_act))
            rounded = values.astype(jnp.bfloat16)
            target[:, block] = rounded
            values = rounded.astype(jnp.float32)
            return squares + values * values

        return scale_inv(sweep(body, flat))

    near_rows(0)
    gather_columns(0)
    columns_ready(0)
    act[0, :, cols(own_f)] = matmul(normed[0], wc[0]).astype(jnp.bfloat16)
    gather_start(0)
    gather_forward(0)

    gather_columns(1)

    @pl.when(keeper)
    def _():
        arrived(wr.at[1 - y], wr_recv.at[1 - y])

    send(wr.at[1 - y], wr.at[1 - y], wr_recv.at[1 - y], partner, keeper)
    for dz in range(reps):
        for dx in range(2):
            for dc in range(2):
                if dz or dx or dc:
                    k = lax.rem(z + dz, reps) * 4 + (1 - x if dx else x) * 2 + (1 - core if dc else core)
                    arrived(ids.at[k], ids_recv.at[k])

    token_rows = ids.shape[1] // 2
    counts[...] = jnp.zeros_like(counts)

    def pairs(k, carry):
        block = ids[k]
        rows = own_vocab((half, LANES))
        words = lax.broadcasted_iota(jnp.int32, (vocab, LANES), 0)
        total = counts[...]
        for r in range(token_rows):
            token = (rows == block[r : r + 1]).astype(jnp.float32).astype(jnp.bfloat16)
            target = (words == block[token_rows + r : token_rows + r + 1]).astype(jnp.float32)
            total = total + matmul(token, target.astype(jnp.bfloat16), over_last)
        counts[...] = total
        return carry

    lax.fori_loop(0, members, pairs, 0)
    columns_ready(1)
    gather_finish(0)

    scale[1] = layer_out(x1, x0, act.at[0])
    norm_into(normed.at[1], x1, 1, gains.at[1])
    act[1, :, cols(own_f)] = matmul(normed[1], wc[1]).astype(jnp.bfloat16)
    gather_start(1)
    near_rows(1)
    gather_forward(1)
    gather_finish(1)

    scale[2] = layer_out(x2, x1, act.at[1])
    norm_into(top, x2, 2, final_ref)
    raw = matmul(top[...], emb[...], over_last)
    exp_logit = jnp.exp(raw * logit_scale)
    probability = exp_logit / jnp.sum(exp_logit, axis=-1, keepdims=True)
    pair_counts = counts[...]
    row_counts = jnp.sum(pair_counts, axis=-1, keepdims=True)
    grad_logit = ((row_counts * probability - pair_counts) * logit_scale).astype(jnp.bfloat16)
    grad_wide = grad_logit.astype(jnp.float32)
    qt[...] = jnp.transpose(grad_wide).astype(jnp.bfloat16)
    final_mean = jnp.broadcast_to(
        jnp.sum(grad_wide * raw, axis=-1, keepdims=True) * (1.0 / features), (half, LANES)
    )
    mine = cols(core, half)

    def head_back(block, total):
        grad = matmul(grad_logit, emb[:, block])
        unit = x2[:, block].astype(jnp.float32) * scale[2]
        part[0, :, block] = jnp.sum(grad * unit, axis=0, keepdims=True)
        rounded = (scale[2] * (grad * final_ref[:, block] - unit * final_mean)).astype(jnp.bfloat16)
        dx2[:, block] = rounded
        pre_act = act[1, :, block].astype(jnp.float32)
        pre_grad = (rounded.astype(jnp.float32) * slope(pre_act)).astype(jnp.bfloat16)
        da[1, mine, block] = pre_grad
        return total + pre_grad.astype(jnp.float32) * pre_act

    scale[4] = mean_of(sweep(head_back, flat))

    @pl.when(core == y)
    def _():
        pass

    @pl.when(jnp.logical_not(keeper))
    def _():
        arrived(wr.at[y], wr_recv.at[y])
        arrived(wr.at[1 - y], wr_recv.at[1 - y])

    act[2, :, cols(own_f)] = matmul(da[1, mine], wr[1], over_last).astype(jnp.bfloat16)
    gather_start(2)
    send(da.at[1, mine], da.at[1, mine], misc_recv.at[2], partner, y == 1)
    send(part.at[0], part_in.at[0], misc_recv.at[3], partner)
    gather_forward(2)

    own_group = y * (2 * reps) + z * 2 + x
    for c in range(2):
        hg[c] = matmul(qt[cols(own_group, 2 * group)], top[...])[c * group : (c + 1) * group]
    send(hg.at[1 - core], hg_in, misc_recv.at[4], partner)

    def weight_grad():
        arrived(near.at[cols(1 - core, half)], misc_recv.at[1])
        chunk = 4 * LANES

        def body(j, carry):
            block = cols(j, chunk)
            weight_out[:, block] = matmul(near[...], da[y, :, block], over_first)
            return carry

        lax.fori_loop(0, features // chunk, body, 0)

    @pl.when(y == 1)
    def _():
        arrived(da.at[1, cols(1 - core, half)], misc_recv.at[2])
        weight_grad()

    gather_finish(2)

    def layer_back(block, total):
        grad = act[2, :, block].astype(jnp.float32)
        unit = x1[:, block].astype(jnp.float32) * scale[1]
        part[1, :, block] = jnp.sum(grad * unit, axis=0, keepdims=True)
        inside = scale[1] * (grad * gains[1, :, block] - unit * scale[4])
        rounded = (dx2[:, block].astype(jnp.float32) + inside).astype(jnp.bfloat16)
        dx1[:, block] = rounded
        pre_act = act[0, :, block].astype(jnp.float32)
        pre_grad = (rounded.astype(jnp.float32) * slope(pre_act)).astype(jnp.bfloat16)
        da[0, mine, block] = pre_grad
        return total + pre_grad.astype(jnp.float32) * pre_act

    scale[3] = mean_of(sweep(layer_back, flat))
    grad_norm = matmul(da[0, mine], wr[0], over_last)
    dn0[...] = grad_norm
    unit = x0[:, cols(own_f)].astype(jnp.float32) * scale[0]
    g0[...] = jnp.sum(grad_norm * unit, axis=0, keepdims=True)
    for rel in range(1, chips):
        j = lax.rem(own_group + rel, chips)
        place = {"section": j // (2 * reps), "rep": (j // 2) % reps, "sub": (j % 2) * 2 + core}
        send(dn0.at[cols(j, group)], dn0_in.at[own_f], dn0_recv.at[own_f], place)
    dn0_in[own_f] = dn0[cols(own_group, group)]
    own_slot = core * chips + own_f
    for dz in range(reps):
        for dx in range(2):
            for dc in range(2):
                place = {
                    "section": 0,
                    "rep": lax.rem(z + dz, reps),
                    "sub": (1 - x if dx else x) * 2 + (1 - core if dc else core),
                }
                itself = None if dz or dx or dc else y == 1
                send(g0, g0_in.at[own_slot], g0_recv.at[own_slot], place, itself)
    send(da.at[0, mine], da.at[0, mine], misc_recv.at[2], partner, y == 0)
    send(part.at[1], part_in.at[1], misc_recv.at[5], partner)

    @pl.when(y == 0)
    def _():
        g0_in[own_slot] = g0[...]
        arrived(da.at[0, cols(1 - core, half)], misc_recv.at[2])
        weight_grad()

    arrived(part_in.at[0], misc_recv.at[3])
    final_out[...] = part[0] + part_in[0]
    arrived(hg_in, misc_recv.at[4])
    arrived(part_in.at[1], misc_recv.at[5])

    @pl.when(y == 1)
    def _():
        gain_out[...] = part[1] + part_in[1]

    select = (
        lax.broadcasted_iota(jnp.int32, (group, half), 1)
        == lax.broadcasted_iota(jnp.int32, (group, half), 0) + own_group * group
    ).astype(jnp.float32).astype(jnp.bfloat16)
    own_group_rows = cols(own_group, group)
    row_scale = scale[0, own_group_rows]
    row_mean = scale[3, own_group_rows]

    for rel in range(1, chips):
        f = lax.rem(own_f + rel, chips)
        arrived(dn0_in.at[f], dn0_recv.at[f])

    def finish(f, carry):
        block = cols(f)
        grad = dn0_in[f]
        unit = matmul(select, x0[:, block]) * row_scale[:, :1]
        inside = row_scale[:, :1] * (grad * gains[0, :, block] - unit * row_mean[:, :1])
        total = matmul(select, dx1[:, block]) + inside
        embed_out[:, block] = total.astype(jnp.bfloat16).astype(jnp.float32) + hg[core, :, block] + hg_in[:, block]
        return carry

    lax.fori_loop(0, chips, finish, 0)

    @pl.when(y == 0)
    def _():
        for dz in range(reps):
            for dx in range(2):
                for dy in range(2):
                    for dc in range(2):
                        if dz or dx or dy or dc:
                            f = chip_of(1 - y if dy else y, lax.rem(z + dz, reps), 1 - x if dx else x)
                            slot = (1 - core if dc else core) * chips + f
                            arrived(g0_in.at[slot], g0_recv.at[slot])

        def gain_sum(f, carry):
            gain_out[:, cols(f)] = g0_in[f] + g0_in[chips + f]
            return carry

        lax.fori_loop(0, chips, gain_sum, 0)

    for when, copy in sent:
        if when is None:
            copy.wait_send()
        else:
            pl.when(when)(copy.wait_send)


def row_body(token_ids, target_ids, embedding, section_weight, section_gain, final_gain):
    reps = lax.axis_size("rep")
    members = 4 * reps
    chips = 4 * reps
    features = embedding.shape[1]
    vocab = embedding.shape[0] * members
    half = vocab // 2
    group = vocab // (2 * members)
    depth = section_weight.shape[1]
    width = features // chips
    token_rows = -(-token_ids.size // LANES)
    token_rows += (-token_rows) % (SUBLANES // 2)

    def rows_of(indices):
        flat = indices.reshape(-1)
        flat = jnp.pad(flat, (0, token_rows * LANES - flat.shape[0]), constant_values=-1)
        return flat.reshape(token_rows, LANES)

    ids = jnp.concatenate([rows_of(token_ids), rows_of(target_ids)], axis=0)
    f32, bf16 = jnp.float32, jnp.bfloat16
    messages = 400
    dma = pltpu.SemaphoreType.DMA
    scratch = [
        pltpu.VMEM((vocab, features), bf16),
        pltpu.VMEM((members,) + ids.shape, jnp.int32),
        pltpu.VMEM((2, features, width), bf16),
        pltpu.VMEM((2, width, features), bf16),
        pltpu.VMEM((2, 1, features), f32),
        pltpu.VMEM((half, vocab), f32),
        pltpu.VMEM((half, features), bf16),
        pltpu.VMEM((half, features), bf16),
        pltpu.VMEM((half, features), bf16),
        pltpu.VMEM((2, half, features), bf16),
        pltpu.VMEM((half, features), bf16),
        pltpu.VMEM((3, half, features), bf16),
        pltpu.VMEM((half, features), bf16),
        pltpu.VMEM((half, features), bf16),
        pltpu.VMEM((2, vocab, features), bf16),
        pltpu.VMEM((vocab, depth), bf16),
        pltpu.VMEM((vocab, half), bf16),
        pltpu.VMEM((2, group, features), f32),
        pltpu.VMEM((group, features), f32),
        pltpu.VMEM((half, width), f32),
        pltpu.VMEM((chips, group, width), f32),
        pltpu.VMEM((1, width), f32),
        pltpu.VMEM((2 * chips, 1, width), f32),
        pltpu.VMEM((2, 1, features), f32),
        pltpu.VMEM((2, 1, features), f32),
        pltpu.VMEM((5, half, LANES), f32),
        dma((messages,)),
        dma((2 * members,)),
        dma((members,)),
        dma((members,)),
        dma((3 * chips,)),
        dma((2,)),
        dma((6,)),
        dma((chips,)),
        dma((2 * chips,)),
    ]
    vmem = pl.BlockSpec(memory_space=pltpu.VMEM)
    weight_grad, gain_grad, embed_grad, final_grad = pl.pallas_call(
        functools.partial(row_kernel, reps),
        out_shape=(
            jax.ShapeDtypeStruct((depth, features), f32),
            jax.ShapeDtypeStruct((1, features), f32),
            jax.ShapeDtypeStruct((group, features), f32),
            jax.ShapeDtypeStruct((1, features), f32),
        ),
        in_specs=[vmem] * 5,
        out_specs=(vmem,) * 4,
        scratch_shapes=scratch,
        compiler_params=pltpu.CompilerParams(
            collective_id=1, has_side_effects=True, vmem_limit_bytes=60 * 1024 * 1024
        ),
        name="row_step",
    )(ids, embedding, section_weight[0], section_gain, final_gain[None])
    return weight_grad[None], gain_grad, embed_grad, final_grad[0]


def fits_rows(mesh, weight_shape, vocab):
    sections, reps, subs = (mesh.shape[name] for name in ("section", "rep", "sub"))
    layers, rows, features = weight_shape
    chips = 4 * reps
    group = vocab // (8 * reps)
    return (
        sections == 2
        and subs == 4
        and reps > 1
        and layers == 2
        and rows == features
        and features % (LANES * chips) == 0
        and features // chips == LANES
        and vocab % (64 * reps) == 0
        and group & (group - 1) == 0
        and vocab <= 1024
    )


def solution(mesh):
    in_specs = (
        P(None, ("rep", "sub")),
        P(None, ("rep", "sub")),
        P(("rep", "sub"), None),
        P("section", ("rep", "sub"), None),
        P("section", None),
        P(),
    )
    out_specs = (
        P("section", ("rep", "sub"), None),
        P("section", None),
        P(("section", "rep", "sub"), None),
        P(),
    )

    def step(*arguments):
        by_rows = fits_rows(mesh, arguments[3].shape, arguments[2].shape[0])
        chosen = row_body if by_rows else pipeline_body
        return jax.shard_map(
            chosen, mesh=mesh, in_specs=in_specs, out_specs=out_specs, check_vma=False
        )(*arguments)

    return step
```

```python
import functools
import jax
import jax.numpy as jnp
from jax import lax
from jax.experimental import pallas as pl
from jax.experimental.pallas import tpu as pltpu
from jax.sharding import PartitionSpec as P

epsilon = 1e-06
gelu_coef = 0.7978845608028654
cube_coef = 0.044715


def passed_along(value, axis, steps):
    count = lax.axis_size(axis)
    initial, last = (max(0, -steps), min(count, count - steps))
    return lax.ppermute(value, axis, [(source, source + steps) for source in range(initial, last)])


def gelu(pre_act):
    return (
        0.5
        * pre_act
        * (1.0 + jnp.tanh(gelu_coef * (pre_act + cube_coef * pre_act * pre_act * pre_act)))
    )


def gelu_slope(pre_act):
    inside = gelu_coef * (pre_act + cube_coef * pre_act * pre_act * pre_act)
    tangent = jnp.tanh(inside)
    return 0.5 * (1.0 + tangent) + 0.5 * pre_act * (1.0 - tangent * tangent) * gelu_coef * (
        1.0 + 3.0 * cube_coef * pre_act * pre_act
    )


def normalize(residual, gain_row):
    values = residual.astype(jnp.float32)
    scale_inv = lax.rsqrt(jnp.mean(values * values, axis=-1, keepdims=True) + epsilon)
    normed = values * scale_inv
    return (normed, scale_inv, (normed * gain_row).astype(jnp.bfloat16))


def norm_back(grad_norm, normed, scale_inv, gain_row):
    grad_unit = grad_norm * gain_row
    grad_in = scale_inv * (
        grad_unit - normed * jnp.mean(grad_unit * normed, axis=-1, keepdims=True)
    )
    return (grad_in, jnp.sum(grad_norm * normed, axis=0))


def pick_slot(buffer, slot_index):
    return lax.dynamic_index_in_dim(buffer, slot_index, 0, keepdims=False)


def place_slot(buffer, update, slot_index):
    return lax.dynamic_update_index_in_dim(buffer, update, slot_index, 0)


def pipeline_body(token_ids, target_ids, embedding, section_weight, section_gain, final_gain):
    sections = lax.axis_size("section")
    position = lax.axis_index("section")
    micro_count = token_ids.shape[0]
    row_count = token_ids.shape[1]
    features = embedding.shape[1]
    group_size = lax.axis_size(("rep", "sub"))
    vocab_rows = embedding.shape[0] * group_size
    tick_count = micro_count + sections - 1
    contract_last = (((1,), (1,)), ((), ()))
    contract_first = (((0,), (0,)), ((), ()))
    vocab_table = lax.all_gather(embedding, ("rep", "sub"), axis=0, tiled=True)
    weight = lax.all_gather(section_weight, ("rep", "sub"), axis=1, tiled=True)[0]
    gain_row = section_gain[0]
    is_first = position == 0
    is_last = position == sections - 1
    vocab_iota = jnp.arange(vocab_rows, dtype=jnp.int32)
    onehot_in = (token_ids.reshape(-1)[:, None] == vocab_iota[None, :]).astype(jnp.bfloat16)
    embedded = jnp.dot(onehot_in, vocab_table, preferred_element_type=jnp.float32).astype(
        jnp.bfloat16
    )
    embedded = embedded.reshape(micro_count, row_count, features)
    empty_rows = jnp.zeros((row_count, features), jnp.bfloat16)
    zeros_stash = jnp.zeros((micro_count, row_count, features), jnp.bfloat16)
    zeros_pre = jnp.zeros((micro_count, row_count, features), jnp.float32)

    def forward_tick(carried, tick_index):
        arrived = carried[0]
        buffers = carried[1:]
        offset = tick_index - position
        active = (offset >= 0) & (offset < micro_count)
        slot_index = jnp.clip(offset, 0, micro_count - 1)
        residual = jnp.where(is_first, pick_slot(embedded, slot_index), arrived)

        def forward_compute(kept_activations):
            input_list, rounded_list, preactivation_list, output_list = kept_activations
            normed, scale_inv, rounded = normalize(residual, gain_row)
            pre_act = jnp.dot(rounded, weight, preferred_element_type=jnp.float32)
            returned_value = (residual.astype(jnp.float32) + gelu(pre_act)).astype(jnp.bfloat16)
            kept_activations = (
                place_slot(input_list, residual, slot_index),
                place_slot(rounded_list, rounded, slot_index),
                place_slot(preactivation_list, pre_act, slot_index),
                place_slot(output_list, returned_value, slot_index),
            )
            return (kept_activations, returned_value)

        def forward_bypass(kept_activations):
            return (kept_activations, empty_rows)

        buffers, returned_value = lax.cond(active, forward_compute, forward_bypass, buffers)
        arrived = passed_along(returned_value, "section", 1)
        return ((arrived,) + buffers, None)

    start_state = (empty_rows, zeros_stash, zeros_stash, zeros_pre, zeros_stash)
    final_state, unused_out = lax.scan(
        forward_tick, start_state, jnp.arange(tick_count, dtype=jnp.int32)
    )
    input_list, rounded_list, preactivation_list, output_list = final_state[1:]
    logit_scale = float(features) ** (-0.5)

    def head(finals):
        normed, scale_inv, final_rows = normalize(finals, final_gain)
        logits = (
            lax.dot_general(
                final_rows, vocab_table, contract_last, preferred_element_type=jnp.float32
            )
            * logit_scale
        )
        exp_logit = jnp.exp(logits)
        probability = exp_logit / jnp.sum(exp_logit, axis=-1, keepdims=True)
        onehot_out = (target_ids.reshape(-1)[:, None] == vocab_iota[None, :]).astype(jnp.float32)
        grad_logit = ((probability - onehot_out) * logit_scale).astype(jnp.bfloat16)
        embed_head = lax.dot_general(
            grad_logit, final_rows, contract_first, preferred_element_type=jnp.float32
        )
        grad_final = jnp.dot(grad_logit, vocab_table, preferred_element_type=jnp.float32)
        grad_in, final_part = norm_back(grad_final, normed, scale_inv, final_gain)
        grad_top = grad_in.astype(jnp.bfloat16).reshape(micro_count, row_count, features)
        return (embed_head, grad_top, final_part)

    def no_head(finals):
        return (
            jnp.zeros((vocab_rows, features), jnp.float32),
            zeros_stash,
            jnp.zeros((features,), jnp.float32),
        )

    embed_head, grad_top, final_part = lax.cond(
        is_last, head, no_head, output_list.reshape(-1, features)
    )

    def backward_tick(carried, tick_index):
        arrived = carried[0]
        buffers = carried[1:]
        offset = tick_index - (sections - 1 - position)
        active = (offset >= 0) & (offset < micro_count)
        slot_index = jnp.clip(offset, 0, micro_count - 1)
        grad_out = jnp.where(is_last, pick_slot(grad_top, slot_index), arrived)

        def backward_compute(kept_activations):
            preactivation_gradients, first_row_gradients, gain_accumulated = kept_activations
            grad_float = grad_out.astype(jnp.float32)
            grad_pre = (grad_float * gelu_slope(pick_slot(preactivation_list, slot_index))).astype(
                jnp.bfloat16
            )
            grad_norm = lax.dot_general(
                grad_pre, weight, contract_last, preferred_element_type=jnp.float32
            )
            normed, scale_inv, rounded = normalize(pick_slot(input_list, slot_index), gain_row)
            grad_in, gain_part = norm_back(grad_norm, normed, scale_inv, gain_row)
            sent_output = (grad_float + grad_in).astype(jnp.bfloat16)
            kept_activations = (
                place_slot(preactivation_gradients, grad_pre, slot_index),
                place_slot(first_row_gradients, sent_output, slot_index),
                gain_accumulated + gain_part,
            )
            return (kept_activations, sent_output)

        def backward_bypass(kept_activations):
            return (kept_activations, empty_rows)

        buffers, sent_output = lax.cond(active, backward_compute, backward_bypass, buffers)
        arrived = passed_along(sent_output, "section", -1)
        return ((arrived,) + buffers, None)

    back_state = (empty_rows, zeros_stash, zeros_stash, jnp.zeros((features,), jnp.float32))
    back_final, unused_back = lax.scan(
        backward_tick, back_state, jnp.arange(tick_count, dtype=jnp.int32)
    )
    preactivation_gradients, first_row_gradients, gain_accumulated = back_final[1:]
    pres_flat = preactivation_gradients.reshape(-1, features)
    rounded_flat = rounded_list.reshape(-1, features)
    weight_part = lax.psum_scatter(
        lax.dot_general(
            rounded_flat, pres_flat, contract_first, preferred_element_type=jnp.float32
        ).astype(jnp.bfloat16),
        ("rep", "sub"),
        scatter_dimension=0,
        tiled=True,
    ).astype(jnp.float32)
    gain_total = lax.psum(gain_accumulated, ("rep", "sub"))
    final_total = lax.psum(final_part, ("section", "rep", "sub"))
    embed_in = lax.dot_general(
        onehot_in,
        first_row_gradients.reshape(-1, features),
        contract_first,
        preferred_element_type=jnp.float32,
    )
    contribution = jnp.where(is_first, embed_in, 0.0) + embed_head
    embed_total = lax.psum_scatter(
        contribution, ("section", "rep", "sub"), scatter_dimension=0, tiled=True
    )
    return (weight_part[None], gain_total[None], embed_total, final_total)


LANES = 128
SUBLANES = 8
MESH = pl.DeviceIdType.MESH
over_last = (((1,), (1,)), ((), ()))
over_first = (((0,), (0,)), ((), ()))


def matmul(left, right, dims=(((1,), (0,)), ((), ()))):
    return lax.dot_general(left, right, dims, preferred_element_type=jnp.float32)


def row_kernel(
    reps,
    relays,
    token_hbm,
    target_hbm,
    emb_hbm,
    w_hbm,
    gain_hbm,
    final_hbm,
    near_hbm,
    da_hbm,
    small_hbm,
    near,
    da,
    small,
    token_ref,
    target_ref,
    w_ref,
    final_ref,
    emb,
    ids,
    wc,
    wr,
    gains,
    counts,
    x0,
    x1,
    x2,
    scaled,
    top,
    act,
    slopes,
    dx2,
    dx1,
    qt,
    hg,
    hg_in,
    dn0,
    dn0_in,
    g0,
    g0_in,
    part,
    part_in,
    scale,
    base,
    load_sem,
    send_sem,
    w_recv,
    emb_recv,
    ids_recv,
    act_recv,
    wr_recv,
    da_recv,
    misc_recv,
    dn0_recv,
    g0_recv,
):
    y, z, sub = (lax.axis_index(name) for name in ("section", "rep", "sub"))
    x, core = sub // 2, sub % 2
    chips = 4 * reps
    members = 4 * reps
    own_k = z * 4 + sub
    features = emb.shape[1]
    vocab = emb.shape[0]
    half = vocab // 2
    width = features // chips
    depth = features // members
    group = vocab // (2 * members)
    held = vocab // members
    blocks = features // LANES
    logit_scale = float(features) ** (-0.5)

    def device(dy, dz, dx, other_core=False):
        place = {"section": 1 - y if dy else y, "rep": lax.rem(z + dz, reps)}
        across = 1 - x if dx else x
        place["sub"] = across * 2 + (1 - core if other_core else core)
        return place

    partner = device(0, 0, 0, True)

    def chip_of(ya, za, xa):
        return za * 4 + xa * 2 + ya

    own_f = chip_of(y, z, x)

    def cols(index, size=width):
        return pl.ds(pl.multiple_of(index * size, size), size)

    barrier = pltpu.get_barrier_semaphore()
    count = 0
    for dy in range(2):
        for dz in range(reps):
            for dx in range(2):
                for dc in range(2):
                    if dy or dz or dx or dc:
                        pl.semaphore_signal(
                            barrier, inc=1, device_id=device(dy, dz, dx, bool(dc)), device_id_type=MESH
                        )
                        count += 1
    loads = []
    for number, (source, target) in enumerate(
        (
            (emb_hbm, emb.at[cols(own_k, held)]),
            (w_hbm.at[0], w_ref),
            (gain_hbm, gains.at[y]),
            (token_hbm, token_ref),
            (target_hbm, target_ref),
            (final_hbm, final_ref),
        )
    ):
        loads.append(pltpu.make_async_copy(source, target, load_sem.at[number]))
        loads[-1].start()
    pl.semaphore_wait(barrier, count)

    numbers = [0]
    sent = []

    def message(source, target, recv, place):
        number = numbers[0]
        numbers[0] += 1
        return pltpu.make_async_remote_copy(
            src_ref=source,
            dst_ref=target,
            send_sem=send_sem.at[number],
            recv_sem=recv,
            device_id=place,
            device_id_type=MESH,
        )

    def send(source, target, recv, place, when=None):
        copy = message(source, target, recv, place)
        sent.append((when, copy))
        if when is None:
            copy.start()
        else:
            pl.when(when)(copy.start)

    def arrived(target, recv):
        pltpu.make_async_copy(target, target, recv).wait()

    below, above = z, reps - 1 - z
    both = jnp.minimum(below, above)
    z_near = []
    for step in range(1, reps):
        paired = step <= 2 * both
        hop = jnp.where(paired, (step + 1) // 2, step - both)
        up = jnp.where(paired, step % 2 == 1, above > below)
        z_near.append(jnp.where(up, z + hop, z - hop))

    def at(dy, za, dx, other_core=False):
        place = device(dy, 0, dx, other_core)
        place["rep"] = za
        return place

    def weight_columns(layer, places, when, across=(1, 0)):
        rows = cols(own_k, depth)
        for za in places:
            for dy, dx in [(dy, dx) for dx in across for dy in (1, 0)]:
                if za is z and not dy and not dx:
                    continue
                there = chip_of(1 - y if dy else y, za, 1 - x if dx else x)
                send(
                    w_ref.at[:, cols(there)],
                    wc.at[layer, rows],
                    w_recv.at[layer * members + own_k],
                    at(dy, za, dx),
                    when,
                )

    far_first = list(reversed(z_near))
    first, second_plane = y == 0, y == 1

    loads[0].wait()
    own_rows = emb.at[cols(own_k, held)]
    for za in reversed(z_near):
        send(own_rows, own_rows, emb_recv.at[own_k], at(0, za, 0))
    for there in (device(0, 0, 1), partner):
        send(own_rows, own_rows, emb_recv.at[own_k], there)
    loads[1].wait()
    weight_columns(y, [z], None)
    own = w_ref.at[:, cols(own_f)]
    send(own, wc.at[y, cols(own_k, depth)], w_recv.at[y * members + own_k], partner)
    loads[2].wait()
    send(gains.at[y], gains.at[y], misc_recv.at[0], device(1, 0, 0))
    for load in loads[3:]:
        load.wait()

    def packed(source, target, row):
        entries = source[...].astype(jnp.float32).astype(jnp.bfloat16)
        count, size = entries.shape
        per_row = LANES // size
        total = jnp.zeros((count, LANES), jnp.float32)
        for r in range(per_row):
            place = (
                lax.broadcasted_iota(jnp.int32, (size, LANES), 1)
                == lax.broadcasted_iota(jnp.int32, (size, LANES), 0) + r * size
            ).astype(jnp.float32).astype(jnp.bfloat16)
            choose = (
                lax.broadcasted_iota(jnp.int32, (count, count), 1)
                == lax.broadcasted_iota(jnp.int32, (count, count), 0) * per_row + r
            ).astype(jnp.float32).astype(jnp.bfloat16)
            spread_out = matmul(entries, place).astype(jnp.bfloat16)
            total = total + matmul(choose, spread_out)
        rows = count // per_row
        target[row : row + rows] = total[:rows].astype(jnp.int32)

    wc[y, cols(own_k, depth)] = w_ref[:, cols(own_f)]
    token_rows = token_ref.shape[0] * token_ref.shape[1] // LANES
    packed(token_ref, ids.at[own_k], 0)
    packed(target_ref, ids.at[own_k], token_rows)

    for dz in reversed(range(reps)):
        for dx in (1, 0):
            for dc in (1, 0):
                if dz or dx or dc:
                    send(ids.at[own_k], ids.at[own_k], ids_recv.at[own_k], device(0, dz, dx, bool(dc)))

    keeper = core == y
    other = jnp.logical_not(keeper)
    for step, za in enumerate(z_near):
        k = za * 4 + sub
        block = emb.at[cols(k, held)]
        arrived(block, emb_recv.at[k])
        for there in (device(0, 0, 1), partner):
            send(block, block, emb_recv.at[k], there)
        if step == 0:
            weight_columns(0, far_first, first, (0,))
    weight_columns(0, far_first, first, (1,))

    send(w_ref, wr.at[0], wr_recv.at[0], device(1, 0, 0), jnp.logical_and(other, first))
    send(w_ref, wr.at[y], wr_recv.at[y], partner, keeper)

    for dz in range(reps):
        for dx in range(2):
            for dc in range(2):
                if dz or dx or dc:
                    k = lax.rem(z + dz, reps) * 4 + (1 - x if dx else x) * 2 + (1 - core if dc else core)
                    arrived(ids.at[k], ids_recv.at[k])

    def own_vocab(shape):
        index = lax.broadcasted_iota(jnp.int32, shape, 0)
        return 2 * index - (index & (group - 1)) + core * group

    counts[...] = jnp.zeros_like(counts)

    def pairs(k, carry):
        block = ids[k]
        rows = own_vocab((half, LANES))
        words = lax.broadcasted_iota(jnp.int32, (vocab, LANES), 0)

        def onehot(index, first):
            return jnp.concatenate(
                [
                    (index == block[first + r : first + r + 1]).astype(jnp.float32).astype(jnp.bfloat16)
                    for r in range(token_rows)
                ],
                axis=1,
            )

        counts[...] += matmul(onehot(rows, 0), onehot(words, token_rows), over_last)
        return carry

    lax.fori_loop(0, members, pairs, 0)

    for za in [z] + z_near:
        k = za * 4 + (1 - x) * 2 + core
        block = emb.at[cols(k, held)]
        arrived(block, emb_recv.at[k])
        send(block, block, emb_recv.at[k], partner)
    weight_columns(1, far_first, second_plane)

    @pl.when(keeper)
    def _():
        wr[y] = w_ref[...]

    for za in [z] + z_near:
        for xa in (x, 1 - x):
            k = za * 4 + xa * 2 + 1 - core
            arrived(emb.at[cols(k, held)], emb_recv.at[k])

    pick = (
        lax.broadcasted_iota(jnp.int32, (half, vocab), 1) == own_vocab((half, vocab))
    ).astype(jnp.float32).astype(jnp.bfloat16)

    def sweep(body, start, size=LANES):
        for j in range(features // size):
            start = body(pl.ds(j * size, size), start)
        return start

    flat = jnp.zeros((half, LANES), jnp.float32)

    def folded(values):
        total = values[:, :LANES]
        for j in range(1, values.shape[1] // LANES):
            total = total + values[:, j * LANES : (j + 1) * LANES]
        return total

    def mean_of(total):
        mean = jnp.sum(total, axis=-1, keepdims=True) * (1.0 / features)
        return jnp.broadcast_to(mean, (half, LANES))

    def scale_inv(squares):
        return lax.rsqrt(mean_of(squares) + epsilon)

    arrived(gains.at[1 - y], misc_recv.at[0])

    def look_up(block, squares):
        values = matmul(pick, emb[:, block])
        x0[:, block] = values.astype(jnp.bfloat16)
        scaled[:, block] = (values * gains[0, :, block]).astype(jnp.bfloat16)
        return squares + folded(values * values)

    scale[0] = scale_inv(sweep(look_up, flat, 4 * LANES))

    def near_rows(layer, source):
        rows = cols(core, half)

        def rows_of(index):
            block = cols(index, depth)
            unit = source[:, block].astype(jnp.float32) * scale[layer]
            return (unit * gains[layer, :, block]).astype(jnp.bfloat16)

        @pl.when(y == layer)
        def _():
            near[rows] = rows_of(own_k)
            base[...] = rows_of(z * 4 + x * 2 + 1 - core)

        send(base, near.at[rows], misc_recv.at[1], partner, y == layer)

    def gather_columns(layer):
        for za in [z] + z_near:
            for dx in (0, 1):
                k = za * 4 + (1 - x if dx else x) * 2 + core
                block = wc.at[layer, cols(k, depth)]
                recv = w_recv.at[layer * members + k]
                if za is z and not dx:

                    @pl.when(y != layer)
                    def _():
                        arrived(block, recv)

                    send(block, block, recv, partner, y != layer)
                else:
                    arrived(block, recv)
                    send(block, block, recv, partner)

    def columns_ready(layer):
        for za in range(reps):
            for xa in range(2):
                k = za * 4 + xa * 2 + 1 - core
                arrived(wc.at[layer, cols(k, depth)], w_recv.at[layer * members + k])

    def act_block(slot, f):
        return act.at[slot, :, cols(f)], act_recv.at[slot * chips + f]

    def pass_on(slot, f, places):
        block, recv = act_block(slot, f)
        for dy, dx in places:
            send(block, block, recv, device(dy, 0, dx))

    straight = ((1, 1), (1, 0), (0, 1))
    through = ((1, 0), (0, 1))
    by_x, by_y = relays

    def gather_start(slot):
        block, recv = act_block(slot, own_f)
        for za in reversed(z_near):
            send(block, block, recv, at(0, za, 0))
        pass_on(slot, own_f, through if 0 in by_x + by_y else straight)

    def relay(slot, step, za):
        if step in by_x:
            f = chip_of(y, za, 1 - x)
            arrived(*act_block(slot, f))
            pass_on(slot, f, ((1, 0),))
        if step in by_y:
            f = chip_of(1 - y, za, x)
            arrived(*act_block(slot, f))
            pass_on(slot, f, ((0, 1),))

    def gather_forward(slot):
        for step, za in enumerate(z_near):
            f = chip_of(y, za, x)
            arrived(*act_block(slot, f))
            pass_on(slot, f, through if step + 1 in by_x + by_y else straight)
            relay(slot, step, z if step == 0 else z_near[step - 1])
        relay(slot, reps - 1, z_near[-1])

    def gather_use(slot, use, carry, between=None):
        for za in [z] + z_near:
            carry = use(chip_of(y, za, x), carry)
        step = 0
        for place, za in enumerate([z] + z_near):
            for dy, dx in ((1, 0), (0, 1), (1, 1)):
                f = chip_of(1 - y if dy else y, za, 1 - x if dx else x)
                if between is not None:
                    between(step)
                step += 1
                waited = (place in by_x and (dy, dx) == (0, 1)) or (place in by_y and (dy, dx) == (1, 0))
                if not waited:
                    arrived(*act_block(slot, f))
                carry = use(f, carry)
        return carry

    def cubic(pre_act):
        square = pre_act * pre_act
        tangent = jnp.tanh(gelu_coef * pre_act * (1.0 + cube_coef * square))
        return square, tangent

    def layer_out(slot, target, source, shifted, gain):
        def body(f, squares):
            block = cols(f)
            pre_act = act[slot, :, block].astype(jnp.float32)
            square, tangent = cubic(pre_act)
            gate = 0.5 * (1.0 + tangent)
            values = source[:, block].astype(jnp.float32) + pre_act * gate
            rounded = values.astype(jnp.bfloat16)
            target[:, block] = rounded
            values = rounded.astype(jnp.float32)
            shifted[:, block] = (values * gain[:, block]).astype(jnp.bfloat16)
            slopes[slot, :, block] = gate + 0.5 * pre_act * (1.0 - tangent * tangent) * gelu_coef * (
                1.0 + 3.0 * cube_coef * square
            )
            return squares + values * values

        return body

    gather_columns(0)
    columns_ready(0)
    act[0, :, cols(own_f)] = (matmul(scaled[...], wc[0]) * scale[0][:, :width]).astype(jnp.bfloat16)
    gather_start(0)
    near_rows(0, x0)
    gather_forward(0)

    gather_columns(1)

    send(w_ref, wr.at[1], wr_recv.at[1], device(1, 0, 0), jnp.logical_and(other, second_plane))
    squares = gather_use(0, layer_out(0, x1, x0, scaled, gains.at[1]), flat)

    scale[1] = scale_inv(squares)
    columns_ready(1)
    act[1, :, cols(own_f)] = (matmul(scaled[...], wc[1]) * scale[1][:, :width]).astype(jnp.bfloat16)
    gather_start(1)
    near_rows(1, x1)
    gather_forward(1)

    @pl.when(keeper)
    def _():
        arrived(wr.at[1 - y], wr_recv.at[1 - y])

    send(wr.at[1 - y], wr.at[1 - y], wr_recv.at[1 - y], partner, keeper)
    second = layer_out(1, x2, x1, top, final_ref)

    def second_use(f, carry):
        squares, raw = carry
        block = cols(f)
        squares = second(f, squares)
        return squares, raw + matmul(top[:, block], emb[:, block], over_last)

    squares, raw = gather_use(1, second_use, (flat, jnp.zeros((half, vocab), jnp.float32)))

    scale[2] = scale_inv(squares)
    top_scale = scale[2][:, :1]
    raw = raw * top_scale
    exp_logit = jnp.exp(raw * logit_scale)
    probability = exp_logit / jnp.sum(exp_logit, axis=-1, keepdims=True)
    pair_counts = counts[...]
    row_counts = jnp.sum(pair_counts, axis=-1, keepdims=True)
    grad_logit = ((row_counts * probability - pair_counts) * logit_scale).astype(jnp.bfloat16)
    grad_wide = grad_logit.astype(jnp.float32)
    final_mean = jnp.broadcast_to(
        jnp.sum(grad_wide * raw, axis=-1, keepdims=True) * (1.0 / features), (half, LANES)
    )
    mine = cols(core, half)

    @pl.when(jnp.logical_not(keeper))
    def _():
        arrived(wr.at[y], wr_recv.at[y])
        arrived(wr.at[1 - y], wr_recv.at[1 - y])

    def keep(layer, block, index, values):
        @pl.when(y == layer)
        def _():
            da[mine, block] = values

        send(da.at[mine, block], da.at[mine, block], da_recv.at[index], partner, y == layer)

    def wide(values, size):
        return jnp.concatenate([values] * (size // LANES), axis=1)

    def head_back(block, carry):
        total, grad_in = carry
        grad = matmul(grad_logit, emb[:, block])
        top_wide, mean_wide = (wide(v, block.size) for v in (scale[2], final_mean))
        unit = x2[:, block].astype(jnp.float32) * top_wide
        part[0, :, block] = jnp.sum(grad * unit, axis=0, keepdims=True)
        rounded = (top_wide * (grad * final_ref[:, block] - unit * mean_wide)).astype(jnp.bfloat16)
        dx2[:, block] = rounded
        pre_grad = (rounded.astype(jnp.float32) * slopes[1, :, block]).astype(jnp.bfloat16)
        dx1[:, block] = pre_grad
        total = total + folded(pre_grad.astype(jnp.float32) * act[1, :, block].astype(jnp.float32))
        return total, grad_in + matmul(pre_grad, wr[1, :, block], over_last)

    carry = (flat, jnp.zeros((half, width), jnp.float32))
    carry = sweep(head_back, carry, 4 * LANES)
    act[2, :, cols(own_f)] = carry[1].astype(jnp.bfloat16)
    gather_start(2)
    scale[4] = mean_of(carry[0])
    send(part.at[0], part_in.at[0], misc_recv.at[2], partner)
    for f in range(chips):
        keep(1, pl.ds(f * width, width), f, dx1[:, f * width : (f + 1) * width])
    gather_forward(2)

    qt[...] = jnp.transpose(grad_wide * top_scale).astype(jnp.bfloat16)
    own_group = y * (2 * reps) + z * 2 + x
    for c in range(2):
        hg[c] = matmul(qt[cols(own_group, 2 * group)], top[...])[c * group : (c + 1) * group]
    send(hg.at[1 - core], hg_in, misc_recv.at[3], partner)

    def layer_back(f, carry):
        total, grad_in = carry
        block = cols(f)
        grad = act[2, :, block].astype(jnp.float32)
        unit = x1[:, block].astype(jnp.float32) * scale[1]
        part[1, :, block] = jnp.sum(grad * unit, axis=0, keepdims=True)
        inside = scale[1] * (grad * gains[1, :, block] - unit * scale[4])
        rounded = (dx2[:, block].astype(jnp.float32) + inside).astype(jnp.bfloat16)
        dx1[:, block] = rounded
        pre_grad = (rounded.astype(jnp.float32) * slopes[0, :, block]).astype(jnp.bfloat16)
        keep(0, block, f, pre_grad)
        total = total + pre_grad.astype(jnp.float32) * act[0, :, block].astype(jnp.float32)
        return total, grad_in + matmul(pre_grad, wr[0, :, block], over_last)

    total, grad_norm = gather_use(2, layer_back, (flat, jnp.zeros((half, width), jnp.float32)))
    dn0[...] = grad_norm
    unit = x0[:, cols(own_f)].astype(jnp.float32) * scale[0][:, :width]
    g0[...] = jnp.sum(grad_norm * unit, axis=0, keepdims=True)
    for rel in range(1, chips):
        j = lax.rem(own_group + rel, chips)
        place = {"section": j // (2 * reps), "rep": (j // 2) % reps, "sub": (j % 2) * 2 + core}
        send(dn0.at[cols(j, group)], dn0_in.at[own_f], dn0_recv.at[own_f], place)
    own_slot = core * chips + own_f
    for dz in range(reps):
        for dx in range(2):
            for dc in range(2):
                place = {
                    "section": 0,
                    "rep": lax.rem(z + dz, reps),
                    "sub": (1 - x if dx else x) * 2 + (1 - core if dc else core),
                }
                itself = None if dz or dx or dc else y == 1
                send(g0, g0_in.at[own_slot], g0_recv.at[own_slot], place, itself)
    send(part.at[1], part_in.at[1], misc_recv.at[4], partner)
    scale[3] = mean_of(total)
    dn0_in[own_f] = dn0[cols(own_group, group)]

    @pl.when(y == 0)
    def _():
        g0_in[own_slot] = g0[...]

    select = (
        lax.broadcasted_iota(jnp.int32, (group, half), 1)
        == lax.broadcasted_iota(jnp.int32, (group, half), 0) + own_group * group
    ).astype(jnp.float32).astype(jnp.bfloat16)
    own_group_rows = cols(own_group, group)
    row_scale = scale[0, own_group_rows][:, :1]
    row_mean = scale[3, own_group_rows][:, :1]
    arrived(hg_in, misc_recv.at[3])
    unit = matmul(select, x0[...]) * row_scale
    rest = matmul(select, dx1[...]) - row_scale * unit * row_mean
    hg[core] = hg[core] + hg_in[...] + rest
    arrived(part_in.at[0], misc_recv.at[2])
    arrived(part_in.at[1], misc_recv.at[4])
    small[group + 1 : group + 2] = part[0] + part_in[0]

    @pl.when(y == 1)
    def _():
        small[group : group + 1] = part[1] + part_in[1]

    arrived(near.at[cols(1 - core, half)], misc_recv.at[1])
    for j in range(chips):
        block = da.at[cols(1 - core, half), pl.ds(j * width, width)]
        arrived(block, da_recv.at[j])
    stores = [
        pltpu.make_async_copy(near, near_hbm, load_sem.at[0]),
        pltpu.make_async_copy(da, da_hbm, load_sem.at[1]),
        pltpu.make_async_copy(small, small_hbm, load_sem.at[2]),
    ]
    stores[0].start()
    stores[1].start()

    for rel in range(1, chips):
        f = lax.rem(own_f + rel, chips)
        arrived(dn0_in.at[f], dn0_recv.at[f])
    for f in range(chips):
        block = pl.ds(f * width, width)
        small[:group, block] = hg[core, :, block] + dn0_in[f] * (row_scale * gains[0, :, block])

    @pl.when(y == 0)
    def _():
        for dz in range(reps):
            for dx in range(2):
                for dy in range(2):
                    for dc in range(2):
                        if dz or dx or dy or dc:
                            f = chip_of(1 - y if dy else y, lax.rem(z + dz, reps), 1 - x if dx else x)
                            slot = (1 - core if dc else core) * chips + f
                            arrived(g0_in.at[slot], g0_recv.at[slot])
        for f in range(chips):
            small[group : group + 1, f * width : (f + 1) * width] = g0_in[f] + g0_in[chips + f]

    stores[2].start()
    for when, copy in sent:
        if when is None:
            copy.wait_send()
        else:
            pl.when(when)(copy.wait_send)
    for store in stores:
        store.wait()


def last_kernel(
    steps, near_hbm, da_hbm, small_hbm, weight_hbm, gain_hbm, embed_hbm, final_hbm, near, da, small, weight, sems
):
    group = embed_hbm.shape[0]
    size = da.shape[1] // steps
    blocks = [pl.ds(step * size, size) for step in range(steps)]
    loads = [pltpu.make_async_copy(near_hbm, near, sems.at[0, steps])]
    for step, block in enumerate(blocks):
        loads.append(pltpu.make_async_copy(da_hbm.at[:, block], da.at[:, block], sems.at[0, step]))
    loads.append(pltpu.make_async_copy(small_hbm, small, sems.at[0, steps + 1]))
    for load in loads:
        load.start()
    loads[0].wait()
    copies = []
    for step, block in enumerate(blocks):
        loads[1 + step].wait()
        weight[:, block] = matmul(near[...], da[:, block], over_first)
        copies.append(
            pltpu.make_async_copy(weight.at[:, block], weight_hbm.at[:, block], sems.at[1, step])
        )
        copies[-1].start()
    loads[-1].wait()
    for row, count, target in ((0, group, embed_hbm), (group, 1, gain_hbm), (group + 1, 1, final_hbm)):
        copies.append(
            pltpu.make_async_copy(small.at[pl.ds(row, count)], target, sems.at[1, steps + row - group + 1 if row else steps])
        )
        copies[-1].start()
    for copy in copies:
        copy.wait()


def row_body(token_ids, target_ids, embedding, section_weight, section_gain, final_gain):
    reps = lax.axis_size("rep")
    members = 4 * reps
    chips = 4 * reps
    features = embedding.shape[1]
    vocab = embedding.shape[0] * members
    half = vocab // 2
    group = vocab // (2 * members)
    depth = section_weight.shape[1]
    width = features // chips
    token_rows = token_ids.size // LANES
    f32, bf16 = jnp.float32, jnp.bfloat16
    messages = 400
    dma = pltpu.SemaphoreType.DMA
    small_rows = SUBLANES * (-(-(group + 2) // SUBLANES))
    results = (((vocab, depth), bf16), ((vocab, features), bf16), ((small_rows, features), f32))
    scratch = [pltpu.VMEM(*result) for result in results] + [
        pltpu.VMEM(token_ids.shape, jnp.int32),
        pltpu.VMEM(target_ids.shape, jnp.int32),
        pltpu.VMEM((depth, features), bf16),
        pltpu.VMEM((1, features), f32),
        pltpu.VMEM((vocab, features), bf16),
        pltpu.VMEM((members, 2 * token_rows, LANES), jnp.int32),
        pltpu.VMEM((2, features, width), bf16),
        pltpu.VMEM((2, width, features), bf16),
        pltpu.VMEM((2, 1, features), f32),
        pltpu.VMEM((half, vocab), f32),
        pltpu.VMEM((half, features), bf16),
        pltpu.VMEM((half, features), bf16),
        pltpu.VMEM((half, features), bf16),
        pltpu.VMEM((half, features), bf16),
        pltpu.VMEM((half, features), bf16),
        pltpu.VMEM((3, half, features), bf16),
        pltpu.VMEM((2, half, features), f32),
        pltpu.VMEM((half, features), bf16),
        pltpu.VMEM((half, features), bf16),
        pltpu.VMEM((vocab, half), bf16),
        pltpu.VMEM((2, group, features), f32),
        pltpu.VMEM((group, features), f32),
        pltpu.VMEM((half, width), f32),
        pltpu.VMEM((chips, group, width), f32),
        pltpu.VMEM((1, width), f32),
        pltpu.VMEM((2 * chips, 1, width), f32),
        pltpu.VMEM((2, 1, features), f32),
        pltpu.VMEM((2, 1, features), f32),
        pltpu.VMEM((5, half, LANES), f32),
        pltpu.VMEM((half, depth), bf16),
        dma((6,)),
        dma((messages,)),
        dma((2 * members,)),
        dma((members,)),
        dma((members,)),
        dma((3 * chips,)),
        dma((2,)),
        dma((chips,)),
        dma((5,)),
        dma((chips,)),
        dma((2 * chips,)),
    ]
    hbm = pl.BlockSpec(memory_space=pltpu.HBM)
    near, da, small = pl.pallas_call(
        functools.partial(row_kernel, reps, ((), ())),
        out_shape=tuple(jax.ShapeDtypeStruct(*result) for result in results),
        in_specs=[hbm] * 6,
        out_specs=(hbm,) * 3,
        scratch_shapes=scratch,
        compiler_params=pltpu.CompilerParams(
            collective_id=1, has_side_effects=True, vmem_limit_bytes=62 * 1024 * 1024
        ),
        name="row_step",
    )(token_ids, target_ids, embedding, section_weight, section_gain, final_gain[None])
    steps = 4
    weight_grad, gain_grad, embed_grad, final_grad = pl.pallas_call(
        functools.partial(last_kernel, steps),
        out_shape=(
            jax.ShapeDtypeStruct((depth, features), f32),
            jax.ShapeDtypeStruct((1, features), f32),
            jax.ShapeDtypeStruct((group, features), f32),
            jax.ShapeDtypeStruct((1, features), f32),
        ),
        in_specs=[hbm] * 3,
        out_specs=(hbm,) * 4,
        scratch_shapes=[pltpu.VMEM(*result) for result in results]
        + [pltpu.VMEM((depth, features), f32), dma((2, steps + 3))],
        compiler_params=pltpu.CompilerParams(vmem_limit_bytes=62 * 1024 * 1024),
        name="last_step",
    )(near, da, small)
    return weight_grad[None], gain_grad, embed_grad, final_grad[0]


def fits_rows(mesh, token_shape, weight_shape, vocab):
    sections, reps, subs = (mesh.shape[name] for name in ("section", "rep", "sub"))
    layers, rows, features = weight_shape
    chips = 4 * reps
    micros, columns = token_shape[0], token_shape[1] // chips
    group = vocab // (8 * reps)
    return (
        sections == 2
        and subs == 4
        and reps > 1
        and layers == 2
        and rows == features
        and features % (LANES * chips) == 0
        and features // chips == LANES
        and vocab % (64 * reps) == 0
        and group & (group - 1) == 0
        and vocab <= 256
        and LANES % columns == 0
        and (micros * columns) % LANES == 0
    )


def solution(mesh):
    in_specs = (
        P(None, ("rep", "sub")),
        P(None, ("rep", "sub")),
        P(("rep", "sub"), None),
        P("section", ("rep", "sub"), None),
        P("section", None),
        P(),
    )
    out_specs = (
        P("section", ("rep", "sub"), None),
        P("section", None),
        P(("section", "rep", "sub"), None),
        P(),
    )

    def step(*arguments):
        by_rows = fits_rows(mesh, arguments[0].shape, arguments[3].shape, arguments[2].shape[0])
        chosen = row_body if by_rows else pipeline_body
        return jax.shard_map(
            chosen, mesh=mesh, in_specs=in_specs, out_specs=out_specs, check_vma=False
        )(*arguments)

    return step
```
